32 devices in a mesh: groups: 2 (over y), ctx: 4 (over z), wt: 2 (over x), sub: 2 (over core).
Axes of the slice: x: 2, y: 2, z: 4, core: 2. Of those that a mesh axis runs over, the one named last changes fastest.
Arguments:
- queries: bfloat16 [16, 32, 128, 576], P(('groups', 'ctx'), None, ('wt', 'sub')), parts along dimension 0, may hold values from -80 to 80
- selection: int32 [16, 4, 2], P(('groups', 'ctx')), parts along dimension 0, may hold values from -1 to 15, as said below
- latent_cache: bfloat16 [128, 64, 576], P(('groups', 'ctx')), parts along dimension 0, may hold values from -8 to 8
- value_up: bfloat16 [128, 512, 128], P(None, ('wt', 'sub')), may hold values from -1 to 1
Outputs:
- attended: bfloat16 [16, 32, 128, 128], P(('groups', 'ctx'), None, ('wt', 'sub')), parts along dimension 0
The draws below stay inside these ranges and needn't reach their ends.
There are 2 independent parts, one for each index of `groups`. The reference program is written for one: setup_inputs(seed, part) draws one part's arguments, and reference() takes and returns one part's arrays. A program takes and returns all parts, laid end to end along the dimension named above; an argument that names none is the same for every part. Nothing has to cross between parts.
Inputs may be any that keep to these rules, and one draw needn't show every extreme that they name: `selection`: entry [c, o, s] is the number of a block among the 16 of owner o, or -1 for an empty slot; in an owner's slots live entries come first and differ. Each query block has 4 live entries in all, and in every query block some owner fills all 2 slots.
All inputs are finite; a program needn't handle non-finite values.
Results may differ from the reference program's by a relative error of at most 0.008.
Values may be sent and summed in bfloat16 or wider, within the bound.
A program may use at most 128 MiB of HBM per device.

```python
import jax
import jax.numpy as jnp
from jax import lax

HEADS = 128
LAT = 512
ROPE = 64
NOPE = 128
VDIM = 128
BLK = 64
QC = 32
BLK_OWN = 16
BLOCKS = 64
SPAN_ALL = 8
N_CTX = 4


def build_all(key):
    key_sel = jax.random.fold_in(key, 101)
    key_rank = jax.random.fold_in(key, 202)
    key_cache = jax.random.fold_in(key, 303)
    key_query = jax.random.fold_in(key, 404)
    rankings = jax.vmap(lambda k: jax.random.permutation(k, BLK_OWN))(jax.random.split(key_rank, N_CTX))

    def one_span(span_key):
        first, second, third, fourth = jax.random.split(span_key, 4)
        order = jax.random.permutation(first, N_CTX)
        hottest = jax.random.randint(second, (), 1, N_CTX // 4 + 1)
        position = jnp.zeros((N_CTX,), jnp.int32).at[order].set(jnp.arange(N_CTX, dtype=jnp.int32))
        loads = jnp.where(position < hottest, 2, jnp.where(position < 2 * hottest, 0, 1))
        picks = jnp.min(jax.random.randint(third, (4, N_CTX), 0, BLK_OWN), axis=0)
        jumps = jax.random.randint(fourth, (N_CTX,), 0, BLK_OWN - 1)
        owner_rows = jnp.arange(N_CTX)
        lead = rankings[owner_rows, picks]
        other = rankings[owner_rows, (picks + 1 + jumps) % BLK_OWN]
        slot_zero = jnp.where(loads >= 1, lead, -1)
        slot_one = jnp.where(loads >= 2, other, -1)
        chosen = jnp.stack([slot_zero, slot_one], axis=1).astype(jnp.int32)
        target = (order[0] * BLK_OWN + lead[order[0]]).astype(jnp.int32)
        return (chosen, target)
    selection, targets = jax.vmap(one_span)(jax.random.split(key_sel, SPAN_ALL))
    cache = jnp.clip(jax.random.normal(key_cache, (BLOCKS, BLK, LAT + ROPE), jnp.float32), -6.0, 6.0)
    query = jnp.clip(1.2 * jax.random.normal(key_query, (SPAN_ALL, QC, HEADS, LAT + ROPE), jnp.float32), -7.2, 7.2)
    return (selection, cache, query)


def draw_queries(key, part):
    selection, cache, query = build_all(key)
    return query.astype(jnp.bfloat16)


def draw_selection(key, part):
    selection, cache, query = build_all(key)
    return selection


def draw_latent_cache(key, part):
    selection, cache, query = build_all(key)
    return cache.astype(jnp.bfloat16)


def block_levels(stream_key, dims, shards, low, high):
    loudness, own = 1.0, jax.random.fold_in(stream_key, 6)
    for axis_at, blocks in shards:
        steps = jnp.exp(jax.random.uniform(jax.random.fold_in(own, axis_at), (blocks,), jnp.float32, low / len(shards), high / len(shards)))
        loudness = loudness * jnp.repeat(steps, dims[axis_at] // blocks).reshape([-1 if axis == axis_at else 1 for axis in range(len(dims))])
    return loudness


def noise(rng, dims, width, most, shards=(), kind=jnp.bfloat16):
    entries = width * jax.random.normal(rng, dims, jnp.float32)
    if shards:
        entries = entries * block_levels(rng, dims, shards, -0.22, 0.18)
    return jnp.clip(entries, -most, most).astype(kind)


def setup_inputs(seed: int = 0, part: int = 0) -> dict:
    seeds = jax.random.split(jax.random.key(seed), 5)
    part_splits = jax.random.split(jax.random.fold_in(seeds[4], part), 5)
    queries = draw_queries(jax.random.fold_in(jax.random.fold_in(seeds[4], part), 71), part)
    selection = draw_selection(jax.random.fold_in(jax.random.fold_in(seeds[4], part), 71), part)
    latent_cache = draw_latent_cache(jax.random.fold_in(jax.random.fold_in(seeds[4], part), 71), part)
    value_up = noise(seeds[3], (HEADS, LAT, VDIM), (LAT // 16) ** -0.5, 1.0, ((1, 4),))
    return dict(queries=queries, selection=selection, latent_cache=latent_cache, value_up=value_up)


def one_block(latent_cache, value_up, query, chosen):
    owner_base = (jnp.arange(N_CTX, dtype=jnp.int32) * BLK_OWN)[:, None]
    numbers = (owner_base + jnp.clip(chosen, 0, BLK_OWN - 1)).astype(jnp.int32)
    keys = latent_cache[numbers.reshape(-1)].reshape(-1, LAT + ROPE)
    live = jnp.repeat((chosen >= 0).reshape(-1), BLK)
    rows = query.reshape(-1, LAT + ROPE)
    scores = jnp.einsum("rd,kd->rk", rows, keys, preferred_element_type=jnp.float32)
    scores = scores * jnp.float32((NOPE + ROPE) ** -0.5)
    scores = jnp.where(live[None, :], scores, -jnp.inf)
    expo = jnp.exp(scores - jnp.max(scores, axis=1, keepdims=True))
    totals = jnp.sum(expo, axis=1, keepdims=True)
    weights = expo.astype(jnp.bfloat16)
    latent = (jnp.dot(weights, keys[:, :LAT], preferred_element_type=jnp.float32) / totals).astype(jnp.bfloat16)
    latent = latent.reshape(QC, HEADS, LAT)
    out = jnp.einsum("qhl,hlv->qhv", latent.astype(jnp.float32), value_up.astype(jnp.float32))
    return out.astype(jnp.bfloat16)


def reference(queries, selection, latent_cache, value_up):
    def step(pair):
        return one_block(latent_cache, value_up, pair[0], pair[1])
    return lax.map(step, (queries, selection))
```

```python
import functools

import jax
import jax.numpy as jnp
from jax import lax
from jax.experimental import pallas as pl
from jax.experimental.pallas import tpu as pltpu
from jax.sharding import PartitionSpec as P

LAT = 512
ROPE = 64
NOPE = 128
MESH = pl.DeviceIdType.MESH


def kernel(
    dims, sel_s, sel_v, q_hbm, cache_hbm, up_hbm, out_ref,
    q_v, cache_v, up_v, sel_in, sel_sm, send_v, keys_v, lat_v, res_v, *rest,
):
    (G, C, W, S, spans, per_span, hh, slots, blk, width, R, V, J, stride) = dims
    kbufs = rest[:spans]
    (loc_sem, sel_snd, sel_rcv, sel_loc, x_snd, x_rcv, s_snd, s_rcv, y_snd, y_rcv,
     k_snd, k_rcv, f_snd, f_rcv) = rest[spans:]
    half = slots // S
    hp = hh // G
    hc = hp // J
    RX = (W - 1) * S
    rows = per_span * hh
    N = spans * per_span
    g, c, w, s = (lax.axis_index(a) for a in ("groups", "ctx", "wt", "sub"))
    me = w * S + s

    def heads(part, j):
        return pl.ds(pl.multiple_of(part * hp + j * hc, hc), hc)

    def rowsof(k):
        return pl.ds(pl.multiple_of(k * R, R), R)

    def shift(i, d, n):
        return lax.rem(i + d + n, n)

    locals_ = [
        pltpu.make_async_copy(cache_hbm, cache_v, loc_sem.at[0]),
        pltpu.make_async_copy(q_hbm, q_v, loc_sem.at[1]),
        pltpu.make_async_copy(
            up_hbm.at[pl.ds(pl.multiple_of(me * hh, hh), hh)], up_v.at[:, rowsof(me)], loc_sem.at[2]
        ),
    ]
    for copy in locals_:
        copy.start()

    barrier = pltpu.get_barrier_semaphore()
    count = 0
    for d in range(1, C):
        pl.semaphore_signal(barrier, inc=1, device_id={"ctx": shift(c, d, C)}, device_id_type=MESH)
        count += 1
    for d in range(1, G):
        pl.semaphore_signal(barrier, inc=1, device_id={"groups": shift(g, d, G)}, device_id_type=MESH)
        count += 1
    for dw in range(W):
        for ds in range(S):
            if dw or ds:
                pl.semaphore_signal(
                    barrier, inc=1, device_id={"wt": shift(w, dw, W), "sub": shift(s, ds, S)},
                    device_id_type=MESH,
                )
                count += 1
    pl.semaphore_wait(barrier, count)

    sel_out = []
    for d in range(1, C):
        copy = pltpu.make_async_remote_copy(
            sel_v, sel_in.at[d - 1], sel_snd.at[d - 1], sel_rcv.at[d - 1],
            device_id={"ctx": shift(c, d, C)}, device_id_type=MESH,
        )
        copy.start()
        sel_out.append(copy)

    def x_copy(r, j, sending):
        dw, ds = r // S + 1, r % S
        if sending:
            w2, s2 = shift(w, dw, W), shift(s, ds, S)
            src_k, dst_k = me, w2 * S + s2
        else:
            w2, s2 = shift(w, -dw, W), shift(s, -ds, S)
            src_k, dst_k = w2 * S + s2, me
        start = pl.multiple_of(dst_k * hh + g * hp + j * hc, hc)
        return pltpu.make_async_remote_copy(
            up_hbm.at[pl.ds(start, hc)], up_v.at[heads(g, j), rowsof(src_k)],
            x_snd.at[r, j], x_rcv.at[r, j],
            device_id={"wt": w2, "sub": s2}, device_id_type=MESH,
        )

    def s_copy(ds, sending):
        s2 = shift(s, ds if sending else -ds, S)
        src_s, dst_s = (s, s2) if sending else (s2, s)
        start = pl.multiple_of((w * S + dst_s) * hh, hh)
        return pltpu.make_async_remote_copy(
            up_hbm.at[pl.ds(start, hh)], up_v.at[:, rowsof(w * S + src_s)],
            s_snd.at[ds - 1], s_rcv.at[ds - 1], device_id={"sub": s2}, device_id_type=MESH,
        )

    def y_copy(dg, r, j, sending):
        dw, ds = r // S + 1, r % S
        src_k = shift(w, -dw, W) * S + shift(s, -ds, S)
        g2 = shift(g, dg if sending else -dg, G)
        part = g if sending else g2
        region = up_v.at[heads(part, j), rowsof(src_k)]
        return pltpu.make_async_remote_copy(
            region, region, y_snd.at[dg - 1, r, j], y_rcv.at[dg - 1, r, j],
            device_id={"groups": g2}, device_id_type=MESH,
        )

    for j in range(J):
        for r in range(RX):
            x_copy(r, j, True).start()

    locals_[0].wait()
    for d in range(1, C):
        sel_out[d - 1].wait_recv()
        copy = pltpu.make_async_copy(sel_in.at[d - 1], sel_sm.at[d - 1], sel_loc.at[d - 1])
        copy.start()
        copy.wait()

    def k_copy(d, i, sending):
        p = shift(c, d if sending else -d, C)
        owner = c if sending else p
        first = owner * slots + s * half
        return pltpu.make_async_remote_copy(
            send_v.at[d - 1, i], kbufs[i].at[pl.ds(first, half)],
            k_snd.at[d - 1, i], k_rcv.at[d - 1, i], device_id={"ctx": p}, device_id_type=MESH,
        )

    def f_copy(d, i, ds, sending):
        owner = shift(c, -d, C)
        s2 = shift(s, ds if sending else -ds, S)
        first = owner * slots + (s if sending else s2) * half
        region = kbufs[i].at[pl.ds(first, half)]
        return pltpu.make_async_remote_copy(
            region, region, f_snd.at[d - 1, i, ds - 1], f_rcv.at[d - 1, i, ds - 1],
            device_id={"sub": s2}, device_id_type=MESH,
        )

    for i in range(spans):
        for d in range(1, C):
            for t in range(half):
                entry = sel_sm[C - d - 1, 0, (i * C + c) * slots + s * half + t]
                send_v[d - 1, i, t] = cache_v[jnp.clip(entry, 0, cache_v.shape[0] - 1)]
            k_copy(d, i, True).start()
    for ds in range(1, S):
        s_copy(ds, True).start()
    for i in range(spans):
        for t in range(slots):
            entry = sel_s[0, (i * C + c) * slots + t]
            kbufs[i][c * slots + t] = cache_v[jnp.clip(entry, 0, cache_v.shape[0] - 1)]

    pending = [(r, j) for j in range(J) for r in range(RX)]

    def forward(n):
        for r, j in pending[:n]:
            x_copy(r, j, False).wait_recv()
            for dg in range(1, G):
                y_copy(dg, r, j, True).start()
        del pending[:n]

    locals_[1].wait()
    share = max(1, (RX * J) // 4)
    forward(share)
    scale = jnp.float32((NOPE + ROPE) ** (-0.5))
    tile = 8 * hh
    for i in range(spans):
        for d in range(1, C):
            k_copy(d, i, False).wait_recv()
            for ds in range(1, S):
                f_copy(d, i, ds, True).start()
        for d in range(1, C):
            for ds in range(1, S):
                f_copy(d, i, ds, False).wait_recv()
        total = C * slots

        def find(n, carry):
            rank, picks = carry
            live = sel_s[0, i * total + n] >= 0
            picks = tuple(
                jnp.where(jnp.logical_and(live, rank == at), n, old) for at, old in enumerate(picks)
            )
            return rank + live.astype(jnp.int32), picks

        zero = jnp.int32(0)
        _, picks = lax.fori_loop(0, total, find, (zero, (zero,) * C))
        for at in range(C):
            keys_v[at * blk : (at + 1) * blk, :] = kbufs[i][picks[at]]

        @pl.loop(0, per_span // 8)
        def _(at):
            first = pl.multiple_of(i * rows + at * tile, tile)
            keys = keys_v[...]
            scores = lax.dot_general(
                q_v[pl.ds(first, tile), :], keys, (((1,), (1,)), ((), ())),
                preferred_element_type=jnp.float32,
            ) * scale
            expo = jnp.exp(scores - jnp.max(scores, axis=1, keepdims=True))
            totals = jnp.sum(expo, axis=1, keepdims=True)
            latent = jnp.dot(
                expo.astype(jnp.bfloat16), keys[:, :LAT], preferred_element_type=jnp.float32
            ) / totals
            for l in range(LAT // 128):
                for n in range(8):
                    at_row = pl.multiple_of((i * per_span + at * 8 + n) * stride, 8)
                    lat_v[l, pl.ds(at_row, hh), :] = latent[n * hh : (n + 1) * hh, l * 128 : (l + 1) * 128]

        forward(share)

    forward(len(pending))

    locals_[2].wait()
    for ds in range(1, S):
        s_copy(ds, False).wait_recv()

    def project(first):
        @pl.loop(0, hc)
        def _(n):
            h = first + n
            left = jnp.concatenate(
                [lat_v[l, pl.ds(h, N, stride=stride), :].astype(jnp.bfloat16) for l in range(LAT // 128)],
                axis=1,
            )
            res_v[pl.ds(h, N, stride=stride), :] = jnp.dot(
                left, up_v[h], preferred_element_type=jnp.float32
            )

    for j in range(J):
        project(g * hp + j * hc)
    for dg in range(1, G):
        for j in range(J):
            for r in range(RX):
                y_copy(dg, r, j, False).wait_recv()
            project(shift(g, -dg, G) * hp + j * hc)

    @pl.loop(0, N)
    def _(n):
        out_ref[n] = res_v[pl.ds(pl.multiple_of(n * stride, 8), hh), :].astype(jnp.bfloat16)

    for copy in sel_out:
        copy.wait_send()
    for j in range(J):
        for r in range(RX):
            x_copy(r, j, True).wait_send()
            for dg in range(1, G):
                y_copy(dg, r, j, True).wait_send()
    for ds in range(1, S):
        s_copy(ds, True).wait_send()
    for i in range(spans):
        for d in range(1, C):
            k_copy(d, i, True).wait_send()
            for ds in range(1, S):
                f_copy(d, i, ds, True).wait_send()


def per_device(queries, selection, latent_cache, value_up):
    G, C, W, S = (lax.axis_size(a) for a in ("groups", "ctx", "wt", "sub"))
    spans, per_span, hh, width = queries.shape
    slots = selection.shape[2]
    blk = latent_cache.shape[1]
    R, V = value_up.shape[1:]
    hp = hh // G
    J = min(4, hp)
    stride = hh + 8
    N = spans * per_span
    RX = (W - 1) * S
    half = slots // S
    dims = (G, C, W, S, spans, per_span, hh, slots, blk, width, R, V, J, stride)
    flat = selection.reshape(1, -1)
    flat = jnp.pad(flat, ((0, 0), (0, -flat.shape[1] % 128)))
    lanes = flat.shape[1]
    bf16, dma = jnp.bfloat16, pltpu.SemaphoreType.DMA
    anywhere = pl.BlockSpec(memory_space=pl.ANY)
    out = pl.pallas_call(
        functools.partial(kernel, dims),
        out_shape=jax.ShapeDtypeStruct((N, hh, V), bf16),
        in_specs=[
            pl.BlockSpec(memory_space=pltpu.SMEM), pl.BlockSpec(memory_space=pltpu.VMEM),
            anywhere, anywhere, anywhere,
        ],
        out_specs=pl.BlockSpec(memory_space=pltpu.VMEM),
        scratch_shapes=[
            pltpu.VMEM((N * hh, width), bf16),
            pltpu.VMEM(latent_cache.shape, bf16),
            pltpu.VMEM((hh, LAT, V), bf16),
            pltpu.VMEM((C - 1, 1, lanes), jnp.int32),
            pltpu.SMEM((C - 1, 1, lanes), jnp.int32),
            pltpu.VMEM((C - 1, spans, half, blk, width), bf16),
            pltpu.VMEM((C * blk, width), bf16),
            pltpu.VMEM((LAT // 128, N * stride, 128), jnp.float32),
            pltpu.VMEM((N * stride, V), jnp.float32),
            *[pltpu.VMEM((C * slots, blk, width), bf16) for _ in range(spans)],
            dma((3,)), dma((C - 1,)), dma((C - 1,)), dma((C - 1,)),
            dma((RX, J)), dma((RX, J)), dma((S - 1,)), dma((S - 1,)),
            dma((G - 1, RX, J)), dma((G - 1, RX, J)),
            dma((C - 1, spans)), dma((C - 1, spans)),
            dma((C - 1, spans, S - 1)), dma((C - 1, spans, S - 1)),
        ],
        compiler_params=pltpu.CompilerParams(
            collective_id=0, has_side_effects=True, vmem_limit_bytes=60 * 1024 * 1024
        ),
    )(flat, flat, queries.reshape(N * hh, width), latent_cache, value_up)
    return out.reshape(spans, per_span, hh, V)


def solution(mesh):
    placed = (
        P(("groups", "ctx"), None, ("wt", "sub"), None),
        P(("groups", "ctx"), None, None),
        P(("groups", "ctx"), None, None),
        P(None, ("wt", "sub"), None),
    )
    return jax.shard_map(
        per_device,
        mesh=mesh,
        in_specs=placed,
        out_specs=P(("groups", "ctx"), None, ("wt", "sub"), None),
        check_vma=False,
    )
```

```python
import functools

import jax
import jax.numpy as jnp
from jax import lax
from jax.experimental import pallas as pl
from jax.experimental.pallas import tpu as pltpu
from jax.sharding import PartitionSpec as P

LAT = 512
ROPE = 64
NOPE = 128
MESH = pl.DeviceIdType.MESH


def kernel(
    dims, sel_s, sel_v, q_hbm, cache_hbm, up_hbm, out_ref,
    q_v, cache_v, up_v, sel_in, sel_sm, send_v, keys_v, lat_v, res_v, *rest,
):
    (G, C, W, S, spans, per_span, hh, slots, blk, width, R, V, J, stride) = dims
    kbufs = rest[:spans]
    (loc_sem, sel_snd, sel_rcv, sel_loc, x_snd, x_rcv, s_snd, s_rcv, y_snd, y_rcv,
     k_snd, k_rcv, f_snd, f_rcv) = rest[spans:]
    half = slots // S
    hp = hh // G
    hc = hp // J
    RX = (W - 1) * S
    rows = per_span * hh
    N = spans * per_span
    g, c, w, s = (lax.axis_index(a) for a in ("groups", "ctx", "wt", "sub"))
    me = w * S + s

    def heads(part, j):
        return pl.ds(pl.multiple_of(part * hp + j * hc, hc), hc)

    def rowsof(k):
        return pl.ds(pl.multiple_of(k * R, R), R)

    def shift(i, d, n):
        return lax.rem(i + d + n, n)

    locals_ = [
        pltpu.make_async_copy(cache_hbm, cache_v, loc_sem.at[0]),
        pltpu.make_async_copy(q_hbm, q_v, loc_sem.at[1]),
        pltpu.make_async_copy(
            up_hbm.at[pl.ds(pl.multiple_of(me * hh, hh), hh)], up_v.at[:, rowsof(me)], loc_sem.at[2]
        ),
    ]
    for copy in locals_:
        copy.start()

    barrier = pltpu.get_barrier_semaphore()
    count = 0
    for d in range(1, C):
        pl.semaphore_signal(barrier, inc=1, device_id={"ctx": shift(c, d, C)}, device_id_type=MESH)
        count += 1
    for d in range(1, G):
        pl.semaphore_signal(barrier, inc=1, device_id={"groups": shift(g, d, G)}, device_id_type=MESH)
        count += 1
    for dw in range(W):
        for ds in range(S):
            if dw or ds:
                pl.semaphore_signal(
                    barrier, inc=1, device_id={"wt": shift(w, dw, W), "sub": shift(s, ds, S)},
                    device_id_type=MESH,
                )
                count += 1
    pl.semaphore_wait(barrier, count)

    sel_out = []
    for d in range(1, C):
        copy = pltpu.make_async_remote_copy(
            sel_v, sel_in.at[d - 1], sel_snd.at[d - 1], sel_rcv.at[d - 1],
            device_id={"ctx": shift(c, d, C)}, device_id_type=MESH,
        )
        copy.start()
        sel_out.append(copy)

    def x_copy(r, j, sending):
        dw, ds = r // S + 1, r % S
        if sending:
            w2, s2 = shift(w, dw, W), shift(s, ds, S)
            src_k, dst_k = me, w2 * S + s2
        else:
            w2, s2 = shift(w, -dw, W), shift(s, -ds, S)
            src_k, dst_k = w2 * S + s2, me
        start = pl.multiple_of(dst_k * hh + g * hp + j * hc, hc)
        return pltpu.make_async_remote_copy(
            up_hbm.at[pl.ds(start, hc)], up_v.at[heads(g, j), rowsof(src_k)],
            x_snd.at[r, j], x_rcv.at[r, j],
            device_id={"wt": w2, "sub": s2}, device_id_type=MESH,
        )

    def s_copy(ds, sending):
        s2 = shift(s, ds if sending else -ds, S)
        src_s, dst_s = (s, s2) if sending else (s2, s)
        start = pl.multiple_of((w * S + dst_s) * hh, hh)
        return pltpu.make_async_remote_copy(
            up_hbm.at[pl.ds(start, hh)], up_v.at[:, rowsof(w * S + src_s)],
            s_snd.at[ds - 1], s_rcv.at[ds - 1], device_id={"sub": s2}, device_id_type=MESH,
        )

    def y_copy(dg, r, j, sending):
        dw, ds = r // S + 1, r % S
        src_k = shift(w, -dw, W) * S + shift(s, -ds, S)
        g2 = shift(g, dg if sending else -dg, G)
        part = g if sending else g2
        region = up_v.at[heads(part, j), rowsof(src_k)]
        return pltpu.make_async_remote_copy(
            region, region, y_snd.at[dg - 1, r, j], y_rcv.at[dg - 1, r, j],
            device_id={"groups": g2}, device_id_type=MESH,
        )

    for j in range(J):
        for r in range(RX):
            x_copy(r, j, True).start()

    locals_[0].wait()
    for d in range(1, C):
        sel_out[d - 1].wait_recv()
        copy = pltpu.make_async_copy(sel_in.at[d - 1], sel_sm.at[d - 1], sel_loc.at[d - 1])
        copy.start()
        copy.wait()

    def k_copy(d, i, sending):
        p = shift(c, d if sending else -d, C)
        owner = c if sending else p
        first = owner * slots + s * half
        return pltpu.make_async_remote_copy(
            send_v.at[d - 1, i], kbufs[i].at[pl.ds(first, half)],
            k_snd.at[d - 1, i], k_rcv.at[d - 1, i], device_id={"ctx": p}, device_id_type=MESH,
        )

    def f_copy(d, i, ds, sending):
        owner = shift(c, -d, C)
        s2 = shift(s, ds if sending else -ds, S)
        first = owner * slots + (s if sending else s2) * half
        region = kbufs[i].at[pl.ds(first, half)]
        return pltpu.make_async_remote_copy(
            region, region, f_snd.at[d - 1, i, ds - 1], f_rcv.at[d - 1, i, ds - 1],
            device_id={"sub": s2}, device_id_type=MESH,
        )

    for i in range(spans):
        for d in range(1, C):
            for t in range(half):
                entry = sel_sm[C - d - 1, 0, (i * C + c) * slots + s * half + t]
                send_v[d - 1, i, t] = cache_v[jnp.clip(entry, 0, cache_v.shape[0] - 1)]
            k_copy(d, i, True).start()
    for ds in range(1, S):
        s_copy(ds, True).start()
    for i in range(spans):
        for t in range(slots):
            entry = sel_s[0, (i * C + c) * slots + t]
            kbufs[i][c * slots + t] = cache_v[jnp.clip(entry, 0, cache_v.shape[0] - 1)]

    pending = [(r, j) for j in range(J) for r in range(RX)]

    def forward(n):
        for r, j in pending[:n]:
            x_copy(r, j, False).wait_recv()
            for dg in range(1, G):
                y_copy(dg, r, j, True).start()
        del pending[:n]

    locals_[1].wait()
    forward((RX * J) // 2)
    scale = jnp.float32((NOPE + ROPE) ** (-0.5))
    tile = 8 * hh
    for i in range(spans):
        for d in range(1, C):
            k_copy(d, i, False).wait_recv()
            for ds in range(1, S):
                f_copy(d, i, ds, True).start()
        forward(-(-RX * J // 8))
        for d in range(1, C):
            for ds in range(1, S):
                f_copy(d, i, ds, False).wait_recv()
        total = C * slots

        def find(n, carry):
            rank, picks = carry
            live = sel_s[0, i * total + n] >= 0
            picks = tuple(
                jnp.where(jnp.logical_and(live, rank == at), n, old) for at, old in enumerate(picks)
            )
            return rank + live.astype(jnp.int32), picks

        zero = jnp.int32(0)
        _, picks = lax.fori_loop(0, total, find, (zero, (zero,) * C))
        for at in range(C):
            keys_v[at * blk : (at + 1) * blk, :] = kbufs[i][picks[at]]

        def attend(at):
            first = pl.multiple_of(i * rows + at * tile, tile)
            keys = keys_v[...]
            scores = lax.dot_general(
                q_v[pl.ds(first, tile), :], keys, (((1,), (1,)), ((), ())),
                preferred_element_type=jnp.float32,
            ) * scale
            expo = jnp.exp(scores - jnp.max(scores, axis=1, keepdims=True))
            totals = jnp.sum(expo, axis=1, keepdims=True)
            latent = jnp.dot(
                expo.astype(jnp.bfloat16), keys[:, :LAT], preferred_element_type=jnp.float32
            ) / totals
            for l in range(LAT // 128):
                for n in range(8):
                    at_row = pl.multiple_of((i * per_span + at * 8 + n) * stride, 8)
                    lat_v[l, pl.ds(at_row, hh), :] = latent[n * hh : (n + 1) * hh, l * 128 : (l + 1) * 128]

        steps = per_span // 8
        for part in range(2):
            pl.loop(part * steps // 2, (part + 1) * steps // 2)(attend)
            forward(-(-RX * J // 16))

    forward(len(pending))

    locals_[2].wait()
    for ds in range(1, S):
        s_copy(ds, False).wait_recv()

    def project(first):
        @pl.loop(0, hc)
        def _(n):
            h = first + n
            left = jnp.concatenate(
                [lat_v[l, pl.ds(h, N, stride=stride), :].astype(jnp.bfloat16) for l in range(LAT // 128)],
                axis=1,
            )
            res_v[pl.ds(h, N, stride=stride), :] = jnp.dot(
                left, up_v[h], preferred_element_type=jnp.float32
            )

    for j in range(J):
        project(g * hp + j * hc)
    for dg in range(1, G):
        for j in range(J):
            for r in range(RX):
                y_copy(dg, r, j, False).wait_recv()
            project(shift(g, -dg, G) * hp + j * hc)

    @pl.loop(0, N)
    def _(n):
        out_ref[n] = res_v[pl.ds(pl.multiple_of(n * stride, 8), hh), :].astype(jnp.bfloat16)

    for copy in sel_out:
        copy.wait_send()
    for j in range(J):
        for r in range(RX):
            x_copy(r, j, True).wait_send()
            for dg in range(1, G):
                y_copy(dg, r, j, True).wait_send()
    for ds in range(1, S):
        s_copy(ds, True).wait_send()
    for i in range(spans):
        for d in range(1, C):
            k_copy(d, i, True).wait_send()
            for ds in range(1, S):
                f_copy(d, i, ds, True).wait_send()


def per_device(queries, selection, latent_cache, value_up):
    G, C, W, S = (lax.axis_size(a) for a in ("groups", "ctx", "wt", "sub"))
    spans, per_span, hh, width = queries.shape
    slots = selection.shape[2]
    blk = latent_cache.shape[1]
    R, V = value_up.shape[1:]
    hp = hh // G
    J = min(8, hp)
    stride = hh + 8
    N = spans * per_span
    RX = (W - 1) * S
    half = slots // S
    dims = (G, C, W, S, spans, per_span, hh, slots, blk, width, R, V, J, stride)
    flat = selection.reshape(1, -1)
    flat = jnp.pad(flat, ((0, 0), (0, -flat.shape[1] % 128)))
    lanes = flat.shape[1]
    bf16, dma = jnp.bfloat16, pltpu.SemaphoreType.DMA
    anywhere = pl.BlockSpec(memory_space=pl.ANY)
    out = pl.pallas_call(
        functools.partial(kernel, dims),
        out_shape=jax.ShapeDtypeStruct((N, hh, V), bf16),
        in_specs=[
            pl.BlockSpec(memory_space=pltpu.SMEM), pl.BlockSpec(memory_space=pltpu.VMEM),
            anywhere, anywhere, anywhere,
        ],
        out_specs=pl.BlockSpec(memory_space=pltpu.VMEM),
        scratch_shapes=[
            pltpu.VMEM((N * hh, width), bf16),
            pltpu.VMEM(latent_cache.shape, bf16),
            pltpu.VMEM((hh, LAT, V), bf16),
            pltpu.VMEM((C - 1, 1, lanes), jnp.int32),
            pltpu.SMEM((C - 1, 1, lanes), jnp.int32),
            pltpu.VMEM((C - 1, spans, half, blk, width), bf16),
            pltpu.VMEM((C * blk, width), bf16),
            pltpu.VMEM((LAT // 128, N * stride, 128), jnp.float32),
            pltpu.VMEM((N * stride, V), jnp.float32),
            *[pltpu.VMEM((C * slots, blk, width), bf16) for _ in range(spans)],
            dma((3,)), dma((C - 1,)), dma((C - 1,)), dma((C - 1,)),
            dma((RX, J)), dma((RX, J)), dma((S - 1,)), dma((S - 1,)),
            dma((G - 1, RX, J)), dma((G - 1, RX, J)),
            dma((C - 1, spans)), dma((C - 1, spans)),
            dma((C - 1, spans, S - 1)), dma((C - 1, spans, S - 1)),
        ],
        compiler_params=pltpu.CompilerParams(
            collective_id=0, has_side_effects=True, vmem_limit_bytes=60 * 1024 * 1024
        ),
    )(flat, flat, queries.reshape(N * hh, width), latent_cache, value_up)
    return out.reshape(spans, per_span, hh, V)


def solution(mesh):
    placed = (
        P(("groups", "ctx"), None, ("wt", "sub"), None),
        P(("groups", "ctx"), None, None),
        P(("groups", "ctx"), None, None),
        P(None, ("wt", "sub"), None),
    )
    return jax.shard_map(
        per_device,
        mesh=mesh,
        in_specs=placed,
        out_specs=P(("groups", "ctx"), None, ("wt", "sub"), None),
        check_vma=False,
    )
```

```python
import functools

import jax
import jax.numpy as jnp
from jax import lax
from jax.experimental import pallas as pl
from jax.experimental.pallas import tpu as pltpu
from jax.sharding import PartitionSpec as P

LAT = 512
ROPE = 64
NOPE = 128
MESH = pl.DeviceIdType.MESH


def kernel(
    dims, sel_s, sel_v, q_hbm, cache_hbm, up_hbm, out_ref,
    q_v, cache_v, up_v, sel_in, sel_sm, send_v, keys_v, lat_v, res_v, *rest,
):
    (G, C, W, S, spans, per_span, hh, slots, blk, width, R, V, J, stride, NU, Z) = dims
    kbufs = rest[:spans]
    (loc_sem, sel_snd, sel_rcv, sel_loc, x_snd, x_rcv, s_snd, s_rcv, y_snd, y_rcv,
     k_snd, k_rcv, f_snd, f_rcv, z_snd, z_rcv) = rest[spans:]
    half = slots // S
    hc = hh // NU
    RX = (W - 1) * S
    rows = per_span * hh
    N = spans * per_span
    g, c, w, s = (lax.axis_index(a) for a in ("groups", "ctx", "wt", "sub"))
    me = w * S + s

    odd = lax.rem(c, 2)

    def head(unit):
        return pl.multiple_of((unit + odd * (NU - 1 - 2 * unit)) * hc, hc)

    def heads(part, j):
        return pl.ds(head(part * J + j), hc)

    def rowsof(k):
        return pl.ds(pl.multiple_of(k * R, R), R)

    def shift(i, d, n):
        return lax.rem(i + d + n, n)

    locals_ = [
        pltpu.make_async_copy(cache_hbm, cache_v, loc_sem.at[0]),
        pltpu.make_async_copy(q_hbm, q_v, loc_sem.at[1]),
        pltpu.make_async_copy(
            up_hbm.at[pl.ds(pl.multiple_of(me * hh, hh), hh)], up_v.at[:, rowsof(me)], loc_sem.at[2]
        ),
    ]
    for copy in locals_:
        copy.start()

    barrier = pltpu.get_barrier_semaphore()
    count = 0
    for d in range(1, C):
        pl.semaphore_signal(barrier, inc=1, device_id={"ctx": shift(c, d, C)}, device_id_type=MESH)
        count += 1
    for d in range(1, G):
        pl.semaphore_signal(barrier, inc=1, device_id={"groups": shift(g, d, G)}, device_id_type=MESH)
        count += 1
    for dw in range(W):
        for ds in range(S):
            if dw or ds:
                pl.semaphore_signal(
                    barrier, inc=1, device_id={"wt": shift(w, dw, W), "sub": shift(s, ds, S)},
                    device_id_type=MESH,
                )
                count += 1
    pl.semaphore_wait(barrier, count)

    sel_out = []
    for d in range(1, C):
        copy = pltpu.make_async_remote_copy(
            sel_v, sel_in.at[d - 1], sel_snd.at[d - 1], sel_rcv.at[d - 1],
            device_id={"ctx": shift(c, d, C)}, device_id_type=MESH,
        )
        copy.start()
        sel_out.append(copy)

    def x_copy(r, j, sending):
        dw, ds = r // S + 1, r % S
        if sending:
            w2, s2 = shift(w, dw, W), shift(s, ds, S)
            src_k, dst_k = me, w2 * S + s2
        else:
            w2, s2 = shift(w, -dw, W), shift(s, -ds, S)
            src_k, dst_k = w2 * S + s2, me
        start = pl.multiple_of(dst_k * hh + head(g * J + j), hc)
        return pltpu.make_async_remote_copy(
            up_hbm.at[pl.ds(start, hc)], up_v.at[heads(g, j), rowsof(src_k)],
            x_snd.at[r, j], x_rcv.at[r, j],
            device_id={"wt": w2, "sub": s2}, device_id_type=MESH,
        )

    def s_copy(ds, sending):
        s2 = shift(s, ds if sending else -ds, S)
        src_s, dst_s = (s, s2) if sending else (s2, s)
        start = pl.multiple_of((w * S + dst_s) * hh, hh)
        return pltpu.make_async_remote_copy(
            up_hbm.at[pl.ds(start, hh)], up_v.at[:, rowsof(w * S + src_s)],
            s_snd.at[ds - 1], s_rcv.at[ds - 1], device_id={"sub": s2}, device_id_type=MESH,
        )

    def y_copy(dg, r, j, sending):
        dw, ds = r // S + 1, r % S
        src_k = shift(w, -dw, W) * S + shift(s, -ds, S)
        g2 = shift(g, dg if sending else -dg, G)
        part = g if sending else g2
        region = up_v.at[heads(part, j), rowsof(src_k)]
        return pltpu.make_async_remote_copy(
            region, region, y_snd.at[dg - 1, r, j], y_rcv.at[dg - 1, r, j],
            device_id={"groups": g2}, device_id_type=MESH,
        )

    def z_copy(r, j, sending):
        dw, ds = r // S + 1, r % S
        src_k = shift(w, -dw, W) * S + shift(s, -ds, S)
        region = up_v.at[pl.ds(head(j if sending else NU - 1 - j), hc), rowsof(src_k)]
        return pltpu.make_async_remote_copy(
            region, region, z_snd.at[r, j], z_rcv.at[r, j],
            device_id={"ctx": c + 1 - 2 * odd}, device_id_type=MESH,
        )

    for j in range(J):
        for r in range(RX):
            x_copy(r, j, True).start()

    locals_[0].wait()
    for d in range(1, C):
        sel_out[d - 1].wait_recv()
        copy = pltpu.make_async_copy(sel_in.at[d - 1], sel_sm.at[d - 1], sel_loc.at[d - 1])
        copy.start()
        copy.wait()

    def k_copy(d, i, sending):
        p = shift(c, d if sending else -d, C)
        owner = c if sending else p
        first = owner * slots + s * half
        return pltpu.make_async_remote_copy(
            send_v.at[d - 1, i], kbufs[i].at[pl.ds(first, half)],
            k_snd.at[d - 1, i], k_rcv.at[d - 1, i], device_id={"ctx": p}, device_id_type=MESH,
        )

    def f_copy(d, i, ds, sending):
        owner = shift(c, -d, C)
        s2 = shift(s, ds if sending else -ds, S)
        first = owner * slots + (s if sending else s2) * half
        region = kbufs[i].at[pl.ds(first, half)]
        return pltpu.make_async_remote_copy(
            region, region, f_snd.at[d - 1, i, ds - 1], f_rcv.at[d - 1, i, ds - 1],
            device_id={"sub": s2}, device_id_type=MESH,
        )

    for i in range(spans):
        for d in range(1, C):
            for t in range(half):
                entry = sel_sm[C - d - 1, 0, (i * C + c) * slots + s * half + t]
                send_v[d - 1, i, t] = cache_v[jnp.clip(entry, 0, cache_v.shape[0] - 1)]
            k_copy(d, i, True).start()
    for ds in range(1, S):
        s_copy(ds, True).start()
    for i in range(spans):
        for t in range(slots):
            entry = sel_s[0, (i * C + c) * slots + t]
            kbufs[i][c * slots + t] = cache_v[jnp.clip(entry, 0, cache_v.shape[0] - 1)]

    pending = [(r, j) for j in range(J) for r in range(RX)]

    def forward(n):
        for r, j in pending[:n]:
            x_copy(r, j, False).wait_recv()
            for dg in range(1, G):
                y_copy(dg, r, j, True).start()
            if j < Z:
                pl.when(g == 0)(z_copy(r, j, True).start)
        del pending[:n]

    locals_[1].wait()
    forward((RX * J) // 2)
    for dg in range(1, G):
        @pl.when(g == dg)
        def _():
            for j in range(Z):
                for r in range(RX):
                    y_copy(dg, r, j, False).wait_recv()
                    z_copy(r, j, True).start()
    scale = jnp.float32((NOPE + ROPE) ** (-0.5))
    tile = 8 * hh
    for i in range(spans):
        for d in range(1, C):
            k_copy(d, i, False).wait_recv()
            for ds in range(1, S):
                f_copy(d, i, ds, True).start()
        forward(-(-RX * J // 8))
        for d in range(1, C):
            for ds in range(1, S):
                f_copy(d, i, ds, False).wait_recv()
        total = C * slots

        def find(n, carry):
            rank, picks = carry
            live = sel_s[0, i * total + n] >= 0
            picks = tuple(
                jnp.where(jnp.logical_and(live, rank == at), n, old) for at, old in enumerate(picks)
            )
            return rank + live.astype(jnp.int32), picks

        zero = jnp.int32(0)
        _, picks = lax.fori_loop(0, total, find, (zero, (zero,) * C))
        for at in range(C):
            keys_v[at * blk : (at + 1) * blk, :] = kbufs[i][picks[at]]

        def attend(at):
            first = pl.multiple_of(i * rows + at * tile, tile)
            keys = keys_v[...]
            scores = lax.dot_general(
                q_v[pl.ds(first, tile), :], keys, (((1,), (1,)), ((), ())),
                preferred_element_type=jnp.float32,
            ) * scale
            expo = jnp.exp(scores - jnp.max(scores, axis=1, keepdims=True))
            totals = jnp.sum(expo, axis=1, keepdims=True)
            latent = jnp.dot(
                expo.astype(jnp.bfloat16), keys[:, :LAT], preferred_element_type=jnp.float32
            ) / totals
            for l in range(LAT // 128):
                for n in range(8):
                    at_row = pl.multiple_of((i * per_span + at * 8 + n) * stride, 8)
                    lat_v[l, pl.ds(at_row, hh), :] = latent[n * hh : (n + 1) * hh, l * 128 : (l + 1) * 128]

        steps = per_span // 8
        for part in range(2):
            pl.loop(part * steps // 2, (part + 1) * steps // 2)(attend)
            forward(-(-RX * J // 16))

    forward(len(pending))

    locals_[2].wait()
    for ds in range(1, S):
        s_copy(ds, False).wait_recv()

    def project(first):
        @pl.loop(0, hc)
        def _(n):
            h = first + n
            left = jnp.concatenate(
                [lat_v[l, pl.ds(h, N, stride=stride), :].astype(jnp.bfloat16) for l in range(LAT // 128)],
                axis=1,
            )
            res_v[pl.ds(h, N, stride=stride), :] = jnp.dot(
                left, up_v[h], preferred_element_type=jnp.float32
            )

    for j in range(J):
        project(head(g * J + j))
    for j in range(Z):
        for r in range(RX):
            z_copy(r, j, False).wait_recv()
        project(head(NU - 1 - j))
    for dg in range(1, G):
        for j in range(J):
            for r in range(RX):
                if j < Z:
                    pl.when(g != dg)(y_copy(dg, r, j, False).wait_recv)
                else:
                    y_copy(dg, r, j, False).wait_recv()
            project(head(shift(g, -dg, G) * J + j))

    @pl.loop(0, N)
    def _(n):
        out_ref[n] = res_v[pl.ds(pl.multiple_of(n * stride, 8), hh), :].astype(jnp.bfloat16)

    for copy in sel_out:
        copy.wait_send()
    for j in range(J):
        for r in range(RX):
            x_copy(r, j, True).wait_send()
            if j < Z:
                z_copy(r, j, True).wait_send()
            for dg in range(1, G):
                y_copy(dg, r, j, True).wait_send()
    for ds in range(1, S):
        s_copy(ds, True).wait_send()
    for i in range(spans):
        for d in range(1, C):
            k_copy(d, i, True).wait_send()
            for ds in range(1, S):
                f_copy(d, i, ds, True).wait_send()


def per_device(queries, selection, latent_cache, value_up):
    G, C, W, S = (lax.axis_size(a) for a in ("groups", "ctx", "wt", "sub"))
    spans, per_span, hh, width = queries.shape
    slots = selection.shape[2]
    blk = latent_cache.shape[1]
    R, V = value_up.shape[1:]
    NU = min(16, hh)
    Z = 2 if C % 2 == 0 and (NU - 2) % G == 0 else 0
    J = (NU - Z) // G
    stride = hh + 8
    N = spans * per_span
    RX = (W - 1) * S
    half = slots // S
    dims = (G, C, W, S, spans, per_span, hh, slots, blk, width, R, V, J, stride, NU, Z)
    flat = selection.reshape(1, -1)
    flat = jnp.pad(flat, ((0, 0), (0, -flat.shape[1] % 128)))
    lanes = flat.shape[1]
    bf16, dma = jnp.bfloat16, pltpu.SemaphoreType.DMA
    anywhere = pl.BlockSpec(memory_space=pl.ANY)
    out = pl.pallas_call(
        functools.partial(kernel, dims),
        out_shape=jax.ShapeDtypeStruct((N, hh, V), bf16),
        in_specs=[
            pl.BlockSpec(memory_space=pltpu.SMEM), pl.BlockSpec(memory_space=pltpu.VMEM),
            anywhere, anywhere, anywhere,
        ],
        out_specs=pl.BlockSpec(memory_space=pltpu.VMEM),
        scratch_shapes=[
            pltpu.VMEM((N * hh, width), bf16),
            pltpu.VMEM(latent_cache.shape, bf16),
            pltpu.VMEM((hh, LAT, V), bf16),
            pltpu.VMEM((C - 1, 1, lanes), jnp.int32),
            pltpu.SMEM((C - 1, 1, lanes), jnp.int32),
            pltpu.VMEM((C - 1, spans, half, blk, width), bf16),
            pltpu.VMEM((C * blk, width), bf16),
            pltpu.VMEM((LAT // 128, N * stride, 128), jnp.float32),
            pltpu.VMEM((N * stride, V), jnp.float32),
            *[pltpu.VMEM((C * slots, blk, width), bf16) for _ in range(spans)],
            dma((3,)), dma((C - 1,)), dma((C - 1,)), dma((C - 1,)),
            dma((RX, J)), dma((RX, J)), dma((S - 1,)), dma((S - 1,)),
            dma((G - 1, RX, J)), dma((G - 1, RX, J)),
            dma((C - 1, spans)), dma((C - 1, spans)),
            dma((C - 1, spans, S - 1)), dma((C - 1, spans, S - 1)),
            dma((RX, max(Z, 1))), dma((RX, max(Z, 1))),
        ],
        compiler_params=pltpu.CompilerParams(
            collective_id=0, has_side_effects=True, vmem_limit_bytes=60 * 1024 * 1024
        ),
    )(flat, flat, queries.reshape(N * hh, width), latent_cache, value_up)
    return out.reshape(spans, per_span, hh, V)


def solution(mesh):
    placed = (
        P(("groups", "ctx"), None, ("wt", "sub"), None),
        P(("groups", "ctx"), None, None),
        P(("groups", "ctx"), None, None),
        P(None, ("wt", "sub"), None),
    )
    return jax.shard_map(
        per_device,
        mesh=mesh,
        in_specs=placed,
        out_specs=P(("groups", "ctx"), None, ("wt", "sub"), None),
        check_vma=False,
    )
```
